8 devices in a mesh: emb: 8 (over z, y, x, core).
Axes of the slice: x: 2, y: 2, z: 1, core: 2. Of those that a mesh axis runs over, the one named last changes fastest.
Arguments:
- tok_ids: int32 [8192], P('emb')
- x_in: bfloat16 [8192, 2048], P('emb')
- d_out: bfloat16 [8192, 2048], P('emb')
- ple_tables: bfloat16 [2, 128256, 256], P(None, 'emb')
- w_up: bfloat16 [2, 2048, 8192], replicated
- w_down: bfloat16 [2, 8192, 2048], replicated
- w_gate: bfloat16 [2, 2048, 256], replicated
- w_proj: bfloat16 [2, 256, 2048], replicated
Outputs:
- output 1: bfloat16 [8192, 2048], P('emb')
- output 2: float32 [2, 128256, 256], P(None, 'emb')
- output 3: float32 [2, 2048, 8192], replicated
- output 4: float32 [2, 8192, 2048], replicated
- output 5: float32 [2, 2048, 256], replicated
- output 6: float32 [2, 256, 2048], replicated
All inputs are finite; a program needn't handle non-finite values.
Results may differ from the reference program's by a relative error of at most 0.0119704.
Values are sent between devices in bfloat16 or wider.
A program may use at most 2 GiB of HBM per device.

```python
import math
import jax
import jax.numpy as jnp
from jax import lax

VOCAB_SIZE = 128256
MODEL_DIM = 2048
HIDDEN_DIM = 8192
EMBED_DIM = 256
LAYERS = 2
TOKENS = 8192
SHARDS = 8

ROWS_DEV = VOCAB_SIZE // SHARDS
TOKENS_PER = TOKENS // SHARDS
CAP_ROWS = TOKENS_PER // 4
ROW_BITS = int(math.log2(ROWS_DEV)) + 1
EPS = 1e-6


def draw_ids(key):
    k_hot, k_off, k_row, k_shift, k_perm = jax.random.split(key, 5)
    hot_owner = jax.random.randint(k_hot, (SHARDS, 1), 0, SHARDS)
    start_off = jax.random.randint(k_off, (SHARDS, 1), 0, SHARDS - 1)
    slot_idx = jnp.arange(TOKENS_PER)[None, :]
    spread_owner = (hot_owner + 1 + (start_off + slot_idx - CAP_ROWS) % (SHARDS - 1)) % SHARDS
    owner_dev = jnp.where(slot_idx < CAP_ROWS, hot_owner, spread_owner)
    raw_rows = jax.random.randint(k_row, (SHARDS, TOKENS_PER), 0, ROWS_DEV)
    shift_bits = jax.random.randint(k_shift, (SHARDS, TOKENS_PER), 0, ROW_BITS + 1)
    local_row = jnp.right_shift(raw_rows, shift_bits)
    id_grid = owner_dev * ROWS_DEV + local_row
    id_grid = jax.random.permutation(k_perm, id_grid, axis=1, independent=True)
    return id_grid.reshape(TOKENS).astype(jnp.int32)


def draw_normal(key, shape, scale):
    return (jax.random.normal(key, shape, jnp.float32) * scale).astype(jnp.bfloat16)


def setup_inputs(seed: int = 0) -> dict:
    key_list = jax.random.split(jax.random.key(seed), 8)
    return {
        "tok_ids": draw_ids(key_list[0]),
        "x_in": draw_normal(key_list[1], (TOKENS, MODEL_DIM), 1.0),
        "d_out": draw_normal(key_list[2], (TOKENS, MODEL_DIM), 1.0),
        "ple_tables": draw_normal(key_list[3], (LAYERS, VOCAB_SIZE, EMBED_DIM), 1.0),
        "w_up": draw_normal(key_list[4], (LAYERS, MODEL_DIM, HIDDEN_DIM), MODEL_DIM ** -0.5),
        "w_down": draw_normal(key_list[5], (LAYERS, HIDDEN_DIM, MODEL_DIM), 0.5 * HIDDEN_DIM ** -0.5),
        "w_gate": draw_normal(key_list[6], (LAYERS, MODEL_DIM, EMBED_DIM), MODEL_DIM ** -0.5),
        "w_proj": draw_normal(key_list[7], (LAYERS, EMBED_DIM, MODEL_DIM), 0.35 * EMBED_DIM ** -0.5),
    }


def gelu_tanh(pre_act):
    return jax.nn.gelu(pre_act, approximate=True)


def gelu_back(pre_act, grad_out):
    _, pull_back = jax.vjp(gelu_tanh, pre_act.astype(jnp.float32))
    return pull_back(grad_out.astype(jnp.float32))[0]


def layer_fwd(x_cur, up_mat, down_mat, gate_mat, proj_mat, emb_rows):
    x_wide = x_cur.astype(jnp.float32)
    inv_rms = lax.rsqrt(jnp.mean(x_wide * x_wide, axis=-1, keepdims=True) + EPS)
    normed = (x_wide * inv_rms).astype(jnp.bfloat16)
    hidden = jnp.dot(normed, up_mat, preferred_element_type=jnp.float32).astype(jnp.bfloat16)
    act_out = gelu_tanh(hidden.astype(jnp.float32)).astype(jnp.bfloat16)
    mlp_out = jnp.dot(act_out, down_mat, preferred_element_type=jnp.float32).astype(jnp.bfloat16)
    gate_pre = jnp.dot(normed, gate_mat, preferred_element_type=jnp.float32).astype(jnp.bfloat16)
    gate_act = gelu_tanh(gate_pre.astype(jnp.float32)).astype(jnp.bfloat16)
    mix_rows = (gate_act.astype(jnp.float32) * emb_rows.astype(jnp.float32)).astype(jnp.bfloat16)
    ple_out = jnp.dot(mix_rows, proj_mat, preferred_element_type=jnp.float32).astype(jnp.bfloat16)
    x_next = (x_wide + mlp_out.astype(jnp.float32) + ple_out.astype(jnp.float32)).astype(jnp.bfloat16)
    return x_next, (x_wide, inv_rms, normed, hidden, act_out, gate_pre, gate_act, mix_rows)


def layer_bwd(d_x, saved, emb_rows, up_mat, down_mat, gate_mat, proj_mat):
    x_wide, inv_rms, normed, hidden, act_out, gate_pre, gate_act, mix_rows = saved
    g_out = d_x.astype(jnp.bfloat16)
    d_act = jnp.dot(g_out, down_mat.T, preferred_element_type=jnp.float32).astype(jnp.bfloat16)
    d_hidden = gelu_back(hidden, d_act).astype(jnp.bfloat16)
    d_mix = jnp.dot(g_out, proj_mat.T, preferred_element_type=jnp.float32).astype(jnp.bfloat16)
    d_rows = gate_act.astype(jnp.float32) * d_mix.astype(jnp.float32)
    d_gate_act = (emb_rows.astype(jnp.float32) * d_mix.astype(jnp.float32)).astype(jnp.bfloat16)
    d_gate_pre = gelu_back(gate_pre, d_gate_act).astype(jnp.bfloat16)
    d_norm = jnp.dot(d_hidden, up_mat.T, preferred_element_type=jnp.float32) + jnp.dot(d_gate_pre, gate_mat.T, preferred_element_type=jnp.float32)
    d_x_new = d_x + inv_rms * d_norm - inv_rms ** 3 * x_wide * jnp.mean(d_norm * x_wide, axis=-1, keepdims=True)
    g_up = jnp.dot(normed.T, d_hidden, preferred_element_type=jnp.float32)
    g_down = jnp.dot(act_out.T, g_out, preferred_element_type=jnp.float32)
    g_gate = jnp.dot(normed.T, d_gate_pre, preferred_element_type=jnp.float32)
    g_proj = jnp.dot(mix_rows.T, g_out, preferred_element_type=jnp.float32)
    return d_x_new, (g_up, g_down, g_gate, g_proj), d_rows


def reference(tok_ids, x_in, d_out, ple_tables, w_up, w_down, w_gate, w_proj):
    weights = (w_up, w_down, w_gate, w_proj)
    ids_blocks = tok_ids.reshape(SHARDS, TOKENS_PER)
    x_blocks = x_in.reshape(SHARDS, TOKENS_PER, MODEL_DIM)
    dy_blocks = d_out.reshape(SHARDS, TOKENS_PER, MODEL_DIM)

    def fwd_step(x_cur, layer_in):
        up_mat, down_mat, gate_mat, proj_mat, emb_rows = layer_in
        return layer_fwd(x_cur, up_mat, down_mat, gate_mat, proj_mat, emb_rows)

    def bwd_step(d_x, layer_in):
        saved, up_mat, down_mat, gate_mat, proj_mat, emb_rows = layer_in
        d_x_new, grads, d_rows = layer_bwd(d_x, saved, emb_rows, up_mat, down_mat, gate_mat, proj_mat)
        return d_x_new, (grads, d_rows)

    def block_step(carry, block_in):
        grad_acc, table_acc = carry
        blk_ids, blk_x, blk_dy = block_in
        rows_all = ple_tables[:, blk_ids, :]
        x_last, saved_all = lax.scan(fwd_step, blk_x, weights + (rows_all,))
        _, (grads, d_rows) = lax.scan(bwd_step, blk_dy.astype(jnp.float32), (saved_all,) + weights + (rows_all,), reverse=True)
        grad_acc = tuple(acc_part + new_part for acc_part, new_part in zip(grad_acc, grads))
        table_acc = table_acc.at[:, blk_ids, :].add(d_rows)
        return (grad_acc, table_acc), x_last

    grad_init = tuple(jnp.zeros(weight_mat.shape, jnp.float32) for weight_mat in weights)
    table_init = jnp.zeros(ple_tables.shape, jnp.float32)
    (grad_acc, table_acc), x_done = lax.scan(block_step, (grad_init, table_init), (ids_blocks, x_blocks, dy_blocks))
    x_out = x_done.reshape(TOKENS, MODEL_DIM)
    return (x_out, table_acc, grad_acc[0], grad_acc[1], grad_acc[2], grad_acc[3])
```

```python
import jax
import jax.numpy as jnp
from jax import lax
from jax.experimental import pallas as pl
from jax.experimental.pallas import tpu as pltpu
from jax.sharding import PartitionSpec as P

EPS = 1e-6
CAP_DIV = 4
BF = jnp.bfloat16
F32 = jnp.float32
SUB = 2


PERM_P = [(i, i ^ (2 if i % 2 == 0 else 4)) for i in range(8)]
PERM_Q = [(i, i ^ (4 if i % 2 == 0 else 2)) for i in range(8)]
PERM_C = [(i, i ^ 1) for i in range(8)]


def hop_p(v):
    return lax.ppermute(v, "emb", PERM_P)


def hop_q(v):
    return lax.ppermute(v, "emb", PERM_Q)


def hop_c(v):
    return lax.ppermute(v, "emb", PERM_C)


def gelu_tanh(pre_act):
    return jax.nn.gelu(pre_act, approximate=True)


def gelu_back(pre_act, grad_out):
    _, pull_back = jax.vjp(gelu_tanh, pre_act.astype(F32))
    return pull_back(grad_out.astype(F32))[0]


def dot_nn(a, b):
    return jnp.dot(a, b, preferred_element_type=F32)


def dot_nt(a, b):
    return lax.dot_general(a, b, (((1,), (1,)), ((), ())), preferred_element_type=F32)


def dot_tn(a, b):
    return lax.dot_general(a, b, (((0,), (0,)), ((), ())), preferred_element_type=F32)


def cut(v, start, size, axis):
    return lax.dynamic_slice_in_dim(v, start, size, axis)


def place_kernel(pos_ref, blk_ref, *rest):
    out_ref = rest[-1]
    out_ref[0] = blk_ref[...].astype(F32)


def place(out, blk, shape, pos):
    rows, cols = blk.shape
    tr = min(rows, 256)
    grid = (rows // tr,)
    per = rows // tr
    in_specs = [pl.BlockSpec((tr, cols), lambda i, s: (i, 0))]
    args = [blk]
    aliases = {}
    if out is not None:
        in_specs.append(pl.BlockSpec(memory_space=pl.ANY))
        args.append(out)
        aliases = {2: 0}
    return pl.pallas_call(
        place_kernel,
        out_shape=jax.ShapeDtypeStruct(shape, F32),
        grid_spec=pltpu.PrefetchScalarGridSpec(
            num_scalar_prefetch=1,
            grid=grid,
            in_specs=in_specs,
            out_specs=pl.BlockSpec((1, tr, cols), lambda i, s: (s[0], s[1] * per + i, s[2])),
        ),
        input_output_aliases=aliases,
        cost_estimate=pl.CostEstimate(flops=rows * cols * 200, bytes_accessed=rows * cols * 6, transcendentals=0),
        name="place",
    )(jnp.stack([jnp.asarray(v, jnp.int32) for v in pos]), *args)


def solution(mesh):
    shards = mesh.shape["emb"]

    def device_step(tok_ids, x_in, d_out, ple_tables, w_up, w_down, w_gate, w_proj):
        layers, rows_dev, emb = ple_tables.shape
        dim, hid = w_up.shape[1:]
        toks = tok_ids.shape[0]
        cap = toks // CAP_DIV
        half, quart, part = hid // 2, hid // 4, hid // 8
        sub = dim // SUB
        me = lax.axis_index("emb")
        core = me % 2
        xb = (me // 2) % 2
        yb = me // 4
        pb = jnp.where(core == 0, xb, yb)
        qb = jnp.where(core == 0, yb, xb)

        def gather_blocks(v):
            got_q = hop_q(v)
            got_p = hop_p(v)
            got_pq = hop_p(got_q)
            mine = [v, got_q, got_p, got_pq]
            return mine + [hop_c(b) for b in mine]

        spot = [core * 4 + (pb ^ i) * 2 + (qb ^ j) for i, j in ((0, 0), (0, 1), (1, 0), (1, 1))]
        oc, op, oq = 1 - core, qb, pb
        spot += [oc * 4 + (op ^ i) * 2 + (oq ^ j) for i, j in ((0, 0), (0, 1), (1, 0), (1, 1))]

        owner_dev = tok_ids // rows_dev
        local_row = tok_ids - owner_dev * rows_dev
        owner_hot = (owner_dev[:, None] == jnp.arange(shards, dtype=jnp.int32)[None, :]).astype(jnp.int32)
        slot_rank = jnp.sum((jnp.cumsum(owner_hot, axis=0) - owner_hot) * owner_hot, axis=1)
        dest_slot = owner_dev * cap + slot_rank
        req_send = jnp.zeros((shards * cap,), jnp.int32).at[dest_slot].set(local_row)
        req_recv = lax.all_to_all(req_send, "emb", 0, 0, tiled=True)
        flat_tables = ple_tables.reshape(layers * rows_dev, emb)
        emb_rows = []
        for l in range(layers):
            served = jnp.take(flat_tables, req_recv + l * rows_dev, axis=0)
            returned = lax.all_to_all(served, "emb", 0, 0, tiled=True)
            emb_rows.append(jnp.take(returned, dest_slot, axis=0))

        def norm(x):
            xw = x.astype(F32)
            r = lax.rsqrt(jnp.mean(xw * xw, axis=-1, keepdims=True) + EPS)
            return xw, r, (xw * r).astype(BF)

        def gate_fwd(u, l):
            z = dot_nn(u, w_gate[l]).astype(BF)
            g = gelu_tanh(z.astype(F32)).astype(BF)
            s = (g.astype(F32) * emb_rows[l].astype(F32)).astype(BF)
            q = dot_nn(s, w_proj[l]).astype(BF)
            return z, g, s, q

        def gate_bwd(o, z, g, l):
            ds = dot_nt(o, w_proj[l]).astype(BF)
            d_rows = g.astype(F32) * ds.astype(F32)
            dg = (emb_rows[l].astype(F32) * ds.astype(F32)).astype(BF)
            dz = gelu_back(z, dg).astype(BF)
            return d_rows, dz

        o1 = d_out
        o1_blocks = gather_blocks(o1)
        x0w, r0, u0 = norm(x_in)
        h0 = dot_nn(u0, w_up[0]).astype(BF)
        a0 = gelu_tanh(h0.astype(F32)).astype(BF)
        z0, g0, s0, q0 = gate_fwd(u0, 0)
        m0 = dot_nn(a0, w_down[0]).astype(BF)
        x1 = (x0w + m0.astype(F32) + q0.astype(F32)).astype(BF)
        x1w, r1, u1 = norm(x1)
        u1_blocks = gather_blocks(u1)
        h1 = dot_nn(u1, w_up[1]).astype(BF)
        z1, g1, s1, q1 = gate_fwd(u1, 1)
        dh1 = gelu_back(h1, dot_nt(o1, w_down[1]).astype(BF)).astype(BF)
        rows1, dz1 = gate_bwd(o1, z1, g1, 1)
        du1 = dot_nt(dh1, w_up[1]) + dot_nt(dz1, w_gate[1])
        c0 = d_out.astype(F32) + r1 * du1 - r1**3 * x1w * jnp.mean(du1 * x1w, axis=-1, keepdims=True)
        o0 = c0.astype(BF)
        dh0 = gelu_back(h0, dot_nt(o0, w_down[0]).astype(BF)).astype(BF)
        rows0, dz0 = gate_bwd(o0, z0, g0, 0)

        up_shape = (layers, dim, hid)
        down_shape = (layers, hid, dim)

        def spread_blocks(block):
            got_q = hop_q(block)
            mine = [block, got_q, hop_p(block), hop_p(got_q)]
            return mine + [hop_c(b) for b in mine]

        def reduce_down(lo):
            o = o0[:, lo : lo + sub]
            piece = lambda start, size: dot_tn(cut(a0, start, size, 1), o)
            mine, keep = core * half, pb * quart
            got = hop_c(piece((1 - core) * half, half).astype(BF))
            go = (1 - pb) * quart
            got_p = hop_p((piece(mine + go, quart) + cut(got, go, quart, 0).astype(F32)).astype(BF))

            def two(off):
                return piece(mine + keep + off, part) + cut(got, keep + off, part, 0).astype(F32) + cut(got_p, off, part, 0).astype(F32)

            got_q = hop_q(two((1 - qb) * part).astype(BF))
            return (two(qb * part) + got_q.astype(F32)).astype(BF)

        def reduce_up(lo):
            u = u0[:, lo : lo + sub]
            piece = lambda start, size: dot_tn(u, cut(dh0, start, size, 1))
            mine, keep = core * half, pb * quart
            got = hop_c(piece((1 - core) * half, half).astype(BF))
            go = (1 - pb) * quart
            got_p = hop_p((piece(mine + go, quart) + cut(got, go, quart, 1).astype(F32)).astype(BF))

            def two(off):
                return piece(mine + keep + off, part) + cut(got, keep + off, part, 1).astype(F32) + cut(got_p, off, part, 1).astype(F32)

            got_q = hop_q(two((1 - qb) * part).astype(BF))
            return (two(qb * part) + got_q.astype(F32)).astype(BF)

        todo = []
        for k in range(SUB):
            todo.append(("down", 0, k, reduce_down(k * sub)))
        for k in range(SUB):
            todo.append(("up", 0, k, reduce_up(k * sub)))

        u_all = jnp.concatenate(u1_blocks, axis=0)
        o_all = jnp.concatenate(o1_blocks, axis=0)
        wu = cut(w_up[1], spot[0] * part, part, 1)
        wd = cut(w_down[1], spot[0] * part, part, 0)
        hs = dot_nn(u_all, wu).astype(BF)
        as_ = gelu_tanh(hs.astype(F32)).astype(BF)
        dhs = gelu_back(hs, dot_nt(o_all, wd).astype(BF)).astype(BF)
        for k in range(SUB):
            todo.append(("down", 1, k, dot_tn(as_, o_all[:, k * sub : (k + 1) * sub]).astype(BF)))
        for k in range(SUB):
            todo.append(("up", 1, k, dot_tn(u_all[:, k * sub : (k + 1) * sub], dhs).astype(BF)))

        g_up = g_down = None
        for kind, l, k, block in todo:
            for where, b in zip(spot, spread_blocks(block)):
                if kind == "down":
                    g_down = place(g_down, b, down_shape, (l, where, k))
                else:
                    g_up = place(g_up, b, up_shape, (l, k, where))

        small = jnp.concatenate([dot_tn(u0, dz0), dot_tn(o0, s0), dot_tn(u1, dz1), dot_tn(o1, s1)], axis=1)
        dh_, dq_, dp_ = dim // 2, dim // 4, dim // 8
        mine = core * dh_
        acc = cut(small, mine, dh_, 0) + hop_c(cut(small, dh_ - mine, dh_, 0).astype(BF)).astype(F32)
        acc = cut(acc, pb * dq_, dq_, 0) + hop_p(cut(acc, (1 - pb) * dq_, dq_, 0).astype(BF)).astype(F32)
        acc = cut(acc, qb * dp_, dp_, 0) + hop_q(cut(acc, (1 - qb) * dp_, dp_, 0).astype(BF)).astype(F32)
        blocks = spread_blocks(acc.astype(BF))
        full = jnp.zeros((dim, 4 * emb), BF)
        for where, b in zip(spot, blocks):
            full = lax.dynamic_update_slice_in_dim(full, b, where * dp_, 0)
        full = full.astype(F32)
        g_gate = jnp.stack([full[:, :emb], full[:, 2 * emb : 3 * emb]])
        g_proj = jnp.stack([full[:, emb : 2 * emb].T, full[:, 3 * emb :].T])

        all_rows, all_ids = [], []
        for l, rows in ((0, rows0), (1, rows1)):
            send = jnp.zeros((shards * cap, emb), F32).at[dest_slot].set(rows)
            all_rows.append(lax.all_to_all(send, "emb", 0, 0, tiled=True))
            all_ids.append(req_recv + l * rows_dev)
        g_tab = jax.ops.segment_sum(jnp.concatenate(all_rows), jnp.concatenate(all_ids), num_segments=layers * rows_dev)
        g_tab = g_tab.reshape(layers, rows_dev, emb)

        a1 = gelu_tanh(h1.astype(F32)).astype(BF)
        m1 = dot_nn(a1, w_down[1]).astype(BF)
        x_out = (x1w + m1.astype(F32) + q1.astype(F32)).astype(BF)
        return x_out, g_tab, g_up, g_down, g_gate, g_proj

    return jax.shard_map(
        device_step,
        mesh=mesh,
        in_specs=(P("emb"), P("emb", None), P("emb", None), P(None, "emb", None), P(), P(), P(), P()),
        out_specs=(P("emb", None), P(None, "emb", None), P(), P(), P(), P()),
        check_vma=False,
    )
```

```python
import math

import jax
import jax.numpy as jnp
from jax import lax
from jax.experimental import pallas as pl
from jax.experimental.pallas import tpu as pltpu
from jax.sharding import PartitionSpec as P


EPS = 1e-6
CAP_DIV = 4
BF = jnp.bfloat16
F32 = jnp.float32
GELU_K = (2.0 / math.pi) ** 0.5
GELU_C = 0.044715


PERM_P = [(i, i ^ (2 if i % 2 == 0 else 4)) for i in range(8)]
PERM_Q = [(i, i ^ (4 if i % 2 == 0 else 2)) for i in range(8)]
PERM_C = [(i, i ^ 1) for i in range(8)]


def keep(v):
    return lax.optimization_barrier(v)


def hop(v, perm):
    return lax.ppermute(v, "emb", perm)


def gelu(h):
    h = h.astype(F32)
    return 0.5 * h * (1.0 + jnp.tanh(h * (GELU_K + (GELU_K * GELU_C) * (h * h))))


def gelu_back(h, grad):
    h = h.astype(F32)
    sq = h * h
    t = jnp.tanh(h * (GELU_K + (GELU_K * GELU_C) * sq))
    slope = (0.5 + 0.5 * t) + (h * (1.0 - t * t)) * (0.5 * GELU_K + (1.5 * GELU_K * GELU_C) * sq)
    return slope * grad.astype(F32)


def dot_nn(a, b):
    return jnp.dot(a, b, preferred_element_type=F32)


def dot_nt(a, b):
    return lax.dot_general(a, b, (((1,), (1,)), ((), ())), preferred_element_type=F32)


def dot_tn(a, b):
    return lax.dot_general(a, b, (((0,), (0,)), ((), ())), preferred_element_type=F32)


def cut(v, start, size, axis):
    return lax.dynamic_slice_in_dim(v, start, size, axis)


def place_kernel(blk_ref, *rest):
    rest[-1][0] = blk_ref[0].astype(F32)


def place(out, blocks, shape, layer, along_cols, base=0):
    n, rows, cols = blocks.shape
    tr = min(rows, 512)
    per = rows // tr
    if along_cols:
        out_map = lambda i, d: (layer, base // tr + i, d)
    else:
        out_map = lambda i, d: (layer, d * per + i, 0)
    in_specs = [pl.BlockSpec((1, tr, cols), lambda i, d: (d, i, 0))]
    args = [blocks]
    aliases = {}
    if out is not None:
        in_specs.append(pl.BlockSpec(memory_space=pl.ANY))
        args.append(out)
        aliases = {1: 0}
    return pl.pallas_call(
        place_kernel,
        out_shape=jax.ShapeDtypeStruct(shape, F32),
        grid=(per, n),
        in_specs=in_specs,
        out_specs=pl.BlockSpec((1, tr, cols), out_map),
        input_output_aliases=aliases,
        cost_estimate=pl.CostEstimate(flops=n * rows * cols * 100, bytes_accessed=n * rows * cols * 6, transcendentals=0),
        name="place",
    )(*args)


def place_list_kernel(pos_ref, *refs):
    out_ref = refs[-1]
    for j in range(8):

        @pl.when(pl.program_id(0) == j)
        def _(j=j):
            out_ref[0] = refs[j][...].astype(F32)


def place_list(out, blocks, where, shape, layer):
    rows, cols = blocks[0].shape
    tr = 256
    per = rows // tr

    def in_map(j):
        return lambda b, i, s: (jnp.where(b == j, i, jnp.where(b < j, 0, per - 1)), 0)

    in_specs = [pl.BlockSpec((tr, cols), in_map(j)) for j in range(8)]
    args = list(blocks)
    aliases = {}
    if out is not None:
        in_specs.append(pl.BlockSpec(memory_space=pl.ANY))
        args.append(out)
        aliases = {9: 0}
    return pl.pallas_call(
        place_list_kernel,
        out_shape=jax.ShapeDtypeStruct(shape, F32),
        grid_spec=pltpu.PrefetchScalarGridSpec(
            num_scalar_prefetch=1,
            grid=(8, per),
            in_specs=in_specs,
            out_specs=pl.BlockSpec((1, tr, cols), lambda b, i, s: (layer, s[b] * per + i, 0)),
        ),
        input_output_aliases=aliases,
        cost_estimate=pl.CostEstimate(flops=rows * cols * 800, bytes_accessed=rows * cols * 48, transcendentals=0),
        name="place",
    )(where, *args)


def solution(mesh):
    shards = mesh.shape["emb"]

    def device_step(tok_ids, x_in, d_out, ple_tables, w_up, w_down, w_gate, w_proj):
        layers, rows_dev, emb = ple_tables.shape
        dim, hid = w_up.shape[1:]
        toks = tok_ids.shape[0]
        cap = toks // CAP_DIV
        part = hid // shards
        me = lax.axis_index("emb")
        core = me & 1
        xb = (me >> 1) & 1
        yb = (me >> 2) & 1
        pb = jnp.where(core == 0, xb, yb)
        qb = jnp.where(core == 0, yb, xb)

        owner_dev = tok_ids // rows_dev
        local_row = tok_ids - owner_dev * rows_dev
        owner_hot = (owner_dev[:, None] == jnp.arange(shards, dtype=jnp.int32)[None, :]).astype(jnp.int32)
        slot_rank = jnp.sum((jnp.cumsum(owner_hot, axis=0) - owner_hot) * owner_hot, axis=1)
        dest_slot = owner_dev * cap + slot_rank
        req_send = jnp.zeros((shards * cap,), jnp.int32).at[dest_slot].set(local_row)
        req_recv = lax.all_to_all(req_send, "emb", 0, 0, tiled=True)
        flat_tables = ple_tables.reshape(layers * rows_dev, emb)
        emb_rows = []
        for l in range(layers):
            served = jnp.take(flat_tables, req_recv + l * rows_dev, axis=0)
            returned = lax.all_to_all(served, "emb", 0, 0, tiled=True)
            emb_rows.append(jnp.take(returned, dest_slot, axis=0))

        def norm(x):
            xw = x.astype(F32)
            r = lax.rsqrt(jnp.mean(xw * xw, axis=-1, keepdims=True) + EPS)
            return xw, r, (xw * r).astype(BF)

        def gate_fwd(u, l):
            z = dot_nn(u, w_gate[l]).astype(BF)
            g = gelu(z).astype(BF)
            z, g = keep((z, g))
            s = keep((g.astype(F32) * emb_rows[l].astype(F32)).astype(BF))
            return z, g, s

        def gate_bwd(o, z, g, l):
            ds = dot_nt(o, w_proj[l]).astype(BF)
            d_rows = g.astype(F32) * ds.astype(F32)
            dg = (emb_rows[l].astype(F32) * ds.astype(F32)).astype(BF)
            dz = gelu_back(z, dg).astype(BF)
            return keep((d_rows, dz))

        o1 = d_out
        o1_all = lax.all_gather(o1, "emb", tiled=True)
        u0 = keep(norm(x_in)[2])
        u0_all = lax.all_gather(u0, "emb", tiled=True)
        a0 = keep(gelu(dot_nn(u0, w_up[0]).astype(BF)).astype(BF))
        m0 = keep(dot_nn(a0, w_down[0]).astype(BF))
        z0, g0, s0 = gate_fwd(u0, 0)
        q0 = dot_nn(s0, w_proj[0]).astype(BF)
        x1 = (x_in.astype(F32) + m0.astype(F32) + q0.astype(F32)).astype(BF)
        x1w, r1, u1 = norm(x1)
        x1, r1, u1 = keep((x1, r1, u1))
        x1w = x1.astype(F32)
        u1_all = lax.all_gather(u1, "emb", tiled=True)
        h1 = keep(dot_nn(u1, w_up[1]).astype(BF))
        z1, g1, s1 = gate_fwd(u1, 1)
        dh1 = keep(gelu_back(h1, dot_nt(o1, w_down[1]).astype(BF)).astype(BF))
        rows1, dz1 = gate_bwd(o1, z1, g1, 1)
        du1 = dot_nt(dh1, w_up[1]) + dot_nt(dz1, w_gate[1])
        c0 = d_out.astype(F32) + r1 * du1 - r1**3 * x1w * jnp.mean(du1 * x1w, axis=-1, keepdims=True)
        o0 = keep(c0.astype(BF))
        o0_all = lax.all_gather(o0, "emb", tiled=True)
        rows0, dz0 = gate_bwd(o0, z0, g0, 0)

        def mlp_grads(l, u_all, o_all, cuts):
            wu = lax.dynamic_slice(w_up, (l, 0, me * part), (1, dim, part))[0]
            hs = keep(dot_nn(u_all, wu).astype(BF))
            g_down = keep(dot_tn(gelu(hs).astype(BF), o_all).astype(BF))
            wd = lax.dynamic_slice(w_down, (l, me * part, 0), (1, part, dim))[0]
            dhs = keep(gelu_back(hs, dot_nt(o_all, wd).astype(BF)).astype(BF))
            g_up = []
            for lo, hi in cuts:
                g_up.append(keep(dot_tn(u_all[:, lo:hi], dhs).astype(BF)))
            return g_up, g_down

        last = dim - dim // 4
        up1, down1 = mlp_grads(1, u1_all, o1_all, ((0, dim),))
        up0, down0 = mlp_grads(0, u0_all, o0_all, ((0, last), (last, dim)))

        up_shape = (layers, dim, hid)
        down_shape = (layers, hid, dim)

        def spread(v):
            return lax.all_gather(v, "emb")

        def spread_list(v):
            got_c = hop(v, PERM_C)
            got_q = hop(v, PERM_Q)
            got_p = hop(v, PERM_P)
            got_r = hop(got_q, PERM_P)
            cross = [got_c, hop(got_q, PERM_C), hop(got_p, PERM_C), hop(got_r, PERM_C)]
            return [v, got_q, got_p, got_r] + cross

        p_bit, q_bit = 2 + 2 * core, 4 - 2 * core
        here = [me, me ^ q_bit, me ^ p_bit, me ^ 6]
        there = [me ^ 1, me ^ 1 ^ p_bit, me ^ 1 ^ q_bit, me ^ 7]
        where = jnp.stack(here + there).astype(jnp.int32)

        g_down = place_list(None, spread_list(down1), where, down_shape, 1)
        g_up = place(None, spread(up1[0]), up_shape, 1, True)
        g_down = place_list(g_down, spread_list(down0), where, down_shape, 0)
        g_up = place(g_up, spread(up0[0]), up_shape, 0, True)
        g_up = place(g_up, spread(up0[1]), up_shape, 0, True, last)

        small = jnp.concatenate([dot_tn(u0, dz0), dot_tn(o0, s0), dot_tn(u1, dz1), dot_tn(o1, s1)], axis=1)
        small = lax.optimization_barrier(small)
        d2, d4, d8 = dim // 2, dim // 4, dim // 8
        mine = core * d2
        acc = cut(small, mine, d2, 0) + hop(cut(small, d2 - mine, d2, 0).astype(BF), PERM_C).astype(F32)
        acc = cut(acc, pb * d4, d4, 0) + hop(cut(acc, (1 - pb) * d4, d4, 0).astype(BF), PERM_P).astype(F32)
        acc = cut(acc, qb * d8, d8, 0) + hop(cut(acc, (1 - qb) * d8, d8, 0).astype(BF), PERM_Q).astype(F32)
        full = spread(acc.astype(BF))
        order = [4 * c + (2 * x + y if c == 0 else 2 * y + x) for y in (0, 1) for x in (0, 1) for c in (0, 1)]
        full = jnp.concatenate([full[order.index(k)] for k in range(shards)], axis=0).astype(F32)
        g_gate = jnp.stack([full[:, :emb], full[:, 2 * emb : 3 * emb]])
        g_proj = jnp.stack([full[:, emb : 2 * emb].T, full[:, 3 * emb :].T])

        all_rows, all_ids = [], []
        for l, rows in ((0, rows0), (1, rows1)):
            send = jnp.zeros((shards * cap, emb), F32).at[dest_slot].set(rows)
            all_rows.append(lax.all_to_all(send, "emb", 0, 0, tiled=True))
            all_ids.append(req_recv + l * rows_dev)
        g_tab = jax.ops.segment_sum(jnp.concatenate(all_rows), jnp.concatenate(all_ids), num_segments=layers * rows_dev)
        g_tab = g_tab.reshape(layers, rows_dev, emb)

        a1 = gelu(h1).astype(BF)
        m1 = dot_nn(a1, w_down[1]).astype(BF)
        q1 = keep(dot_nn(s1, w_proj[1]).astype(BF))
        x_out = (x1w + m1.astype(F32) + q1.astype(F32)).astype(BF)
        return x_out, g_tab, g_up, g_down, g_gate, g_proj

    return jax.shard_map(
        device_step,
        mesh=mesh,
        in_specs=(P("emb"), P("emb", None), P("emb", None), P(None, "emb", None), P(), P(), P(), P()),
        out_specs=(P("emb", None), P(None, "emb", None), P(), P(), P(), P()),
        check_vma=False,
    )
```

```python
import math

import jax
import jax.numpy as jnp
from jax import lax
from jax.experimental import pallas as pl
from jax.experimental.pallas import tpu as pltpu
from jax.sharding import PartitionSpec as P


EPS = 1e-6
CAP_DIV = 4
BF = jnp.bfloat16
F32 = jnp.float32
GELU_K = (2.0 / math.pi) ** 0.5
GELU_C = 0.044715


ALL = ("y", "x", "core")
PERM_X = [(i, i ^ 2) for i in range(8)]
PERM_Y = [(i, i ^ 4) for i in range(8)]
PERM_C = [(i, i ^ 1) for i in range(8)]


def keep(v):
    return lax.optimization_barrier(v)


def hop(v, perm):
    return lax.ppermute(v, ALL, perm)


def gelu(h):
    h = h.astype(F32)
    return 0.5 * h * (1.0 + jnp.tanh(h * (GELU_K + (GELU_K * GELU_C) * (h * h))))


def gelu_back(h, grad):
    h = h.astype(F32)
    sq = h * h
    t = jnp.tanh(h * (GELU_K + (GELU_K * GELU_C) * sq))
    slope = (0.5 + 0.5 * t) + (h * (1.0 - t * t)) * (0.5 * GELU_K + (1.5 * GELU_K * GELU_C) * sq)
    return slope * grad.astype(F32)


def dot_nn(a, b):
    return jnp.dot(a, b, preferred_element_type=F32)


def dot_nt(a, b):
    return lax.dot_general(a, b, (((1,), (1,)), ((), ())), preferred_element_type=F32)


def dot_tn(a, b):
    return lax.dot_general(a, b, (((0,), (0,)), ((), ())), preferred_element_type=F32)


def cut(v, start, size, axis):
    return lax.dynamic_slice_in_dim(v, start, size, axis)


def place_kernel(blk_ref, *rest):
    rest[-1][0] = blk_ref[0].astype(F32)


def owned(dev):
    return (dev & 4) + 2 * (dev & 1) + ((dev >> 1) & 1)


def place(out, blocks, shape, layer, where, base=0):
    n, rows, cols = blocks.shape
    tr = min(rows, 512)
    per = rows // tr
    out_map = lambda i, d: (layer, base // tr + i, where(d))
    in_specs = [pl.BlockSpec((1, tr, cols), lambda i, d: (d, i, 0))]
    args = [blocks]
    aliases = {}
    if out is not None:
        in_specs.append(pl.BlockSpec(memory_space=pl.ANY))
        args.append(out)
        aliases = {1: 0}
    return pl.pallas_call(
        place_kernel,
        out_shape=jax.ShapeDtypeStruct(shape, F32),
        grid=(per, n),
        in_specs=in_specs,
        out_specs=pl.BlockSpec((1, tr, cols), out_map),
        input_output_aliases=aliases,
        cost_estimate=pl.CostEstimate(flops=n * rows * cols * 100, bytes_accessed=n * rows * cols * 6, transcendentals=0),
        name="place",
    )(*args)


def place_list_kernel(pos_ref, *refs):
    out_ref = refs[-1]
    for j in range(8):

        @pl.when(pl.program_id(0) == j)
        def _(j=j):
            out_ref[0] = refs[j][...].astype(F32)


def place_list(out, blocks, where, shape, layer):
    rows, cols = blocks[0].shape
    tr = 256
    per = rows // tr

    def in_map(j):
        return lambda b, i, s: (jnp.where(b == j, i, jnp.where(b < j, 0, per - 1)), 0)

    in_specs = [pl.BlockSpec((tr, cols), in_map(j)) for j in range(8)]
    args = list(blocks)
    aliases = {}
    if out is not None:
        in_specs.append(pl.BlockSpec(memory_space=pl.ANY))
        args.append(out)
        aliases = {9: 0}
    return pl.pallas_call(
        place_list_kernel,
        out_shape=jax.ShapeDtypeStruct(shape, F32),
        grid_spec=pltpu.PrefetchScalarGridSpec(
            num_scalar_prefetch=1,
            grid=(8, per),
            in_specs=in_specs,
            out_specs=pl.BlockSpec((1, tr, cols), lambda b, i, s: (layer, s[b] * per + i, 0)),
        ),
        input_output_aliases=aliases,
        cost_estimate=pl.CostEstimate(flops=rows * cols * 800, bytes_accessed=rows * cols * 48, transcendentals=0),
        name="place",
    )(where, *args)


def solution(mesh):
    shards = mesh.shape["emb"]

    def device_step(tok_ids, x_in, d_out, ple_tables, w_up, w_down, w_gate, w_proj):
        layers, rows_dev, emb = ple_tables.shape
        dim, hid = w_up.shape[1:]
        toks = tok_ids.shape[0]
        cap = toks // CAP_DIV
        part = hid // shards
        me = lax.axis_index(ALL)
        core, x_at, y_at = lax.axis_index("core"), lax.axis_index("x"), lax.axis_index("y")

        owner_dev = tok_ids // rows_dev
        local_row = tok_ids - owner_dev * rows_dev
        owner_hot = (owner_dev[:, None] == jnp.arange(shards, dtype=jnp.int32)[None, :]).astype(jnp.int32)
        slot_rank = jnp.sum((jnp.cumsum(owner_hot, axis=0) - owner_hot) * owner_hot, axis=1)
        dest_slot = owner_dev * cap + slot_rank
        req_send = jnp.zeros((shards * cap,), jnp.int32).at[dest_slot].set(local_row)
        req_recv = lax.all_to_all(req_send, ALL, 0, 0, tiled=True)
        flat_tables = ple_tables.reshape(layers * rows_dev, emb)
        emb_rows = []
        for l in range(layers):
            served = jnp.take(flat_tables, req_recv + l * rows_dev, axis=0)
            returned = lax.all_to_all(served, ALL, 0, 0, tiled=True)
            emb_rows.append(jnp.take(returned, dest_slot, axis=0))

        def norm(x):
            xw = x.astype(F32)
            r = lax.rsqrt(jnp.mean(xw * xw, axis=-1, keepdims=True) + EPS)
            return xw, r, (xw * r).astype(BF)

        def gate_fwd(u, l):
            z = dot_nn(u, w_gate[l]).astype(BF)
            g = gelu(z).astype(BF)
            z, g = keep((z, g))
            s = keep((g.astype(F32) * emb_rows[l].astype(F32)).astype(BF))
            return z, g, s

        def gate_bwd(o, z, g, l):
            ds = dot_nt(o, w_proj[l]).astype(BF)
            d_rows = g.astype(F32) * ds.astype(F32)
            dg = (emb_rows[l].astype(F32) * ds.astype(F32)).astype(BF)
            dz = gelu_back(z, dg).astype(BF)
            return keep((d_rows, dz))

        o1 = d_out
        o1_all = lax.all_gather(o1, ALL, tiled=True)
        u0 = keep(norm(x_in)[2])
        u0_four = lax.all_gather(u0, ("y", "core"), tiled=True)
        a0 = keep(gelu(dot_nn(u0, w_up[0]).astype(BF)).astype(BF))
        m0 = keep(dot_nn(a0, w_down[0]).astype(BF))
        z0, g0, s0 = gate_fwd(u0, 0)
        q0 = dot_nn(s0, w_proj[0]).astype(BF)
        x1 = (x_in.astype(F32) + m0.astype(F32) + q0.astype(F32)).astype(BF)
        x1w, r1, u1 = norm(x1)
        x1, r1, u1 = keep((x1, r1, u1))
        x1w = x1.astype(F32)
        u1_all = lax.all_gather(u1, ALL, tiled=True)
        h1 = keep(dot_nn(u1, w_up[1]).astype(BF))
        z1, g1, s1 = gate_fwd(u1, 1)
        dh1 = keep(gelu_back(h1, dot_nt(o1, w_down[1]).astype(BF)).astype(BF))
        rows1, dz1 = gate_bwd(o1, z1, g1, 1)
        du1 = dot_nt(dh1, w_up[1]) + dot_nt(dz1, w_gate[1])
        c0 = d_out.astype(F32) + r1 * du1 - r1**3 * x1w * jnp.mean(du1 * x1w, axis=-1, keepdims=True)
        o0 = keep(c0.astype(BF))
        o0_four = lax.all_gather(o0, ("y", "core"), tiled=True)
        rows0, dz0 = gate_bwd(o0, z0, g0, 0)

        def hidden(l, u, start, size):
            wu = lax.dynamic_slice(w_up, (l, 0, start), (1, dim, size))[0]
            return keep(dot_nn(u, wu).astype(BF))

        def hidden_back(l, hs, o, start, size):
            wd = lax.dynamic_slice(w_down, (l, start, 0), (1, size, dim))[0]
            return keep(gelu_back(hs, dot_nt(o, wd).astype(BF)).astype(BF))

        hs1 = hidden(1, u1_all, me * part, part)
        down1 = keep(dot_tn(gelu(hs1).astype(BF), o1_all).astype(BF))
        dhs1 = hidden_back(1, hs1, o1_all, me * part, part)
        up1 = keep(dot_tn(u1_all, dhs1).astype(BF))

        quarter = (2 * y_at + core) * 2 * part
        hs0 = hidden(0, u0_four, quarter, 2 * part)
        go, stay = (1 - x_at) * part, x_at * part
        to_x = keep(dot_tn(gelu(cut(hs0, go, part, 1)).astype(BF), o0_four).astype(BF))
        got_d = hop(to_x, PERM_X)
        dhs0 = hidden_back(0, hs0, o0_four, quarter, 2 * part)
        to_x = keep(dot_tn(u0_four, cut(dhs0, go, part, 1)).astype(BF))
        got_u = hop(to_x, PERM_X)
        down0 = keep((dot_tn(gelu(cut(hs0, stay, part, 1)).astype(BF), o0_four) + got_d.astype(F32)).astype(BF))
        up0 = []
        last = dim - dim // 4
        for lo, hi in ((0, last), (last, dim)):
            piece = dot_tn(u0_four[:, lo:hi], cut(dhs0, stay, part, 1)) + got_u[lo:hi].astype(F32)
            up0.append(keep(piece.astype(BF)))

        up_shape = (layers, dim, hid)
        down_shape = (layers, hid, dim)

        def spread(v):
            return lax.all_gather(v, ALL)

        def spread_list(v, first, second):
            got_c = hop(v, PERM_C)
            got_q = hop(v, first)
            got_p = hop(v, second)
            got_r = hop(got_q, second)
            cross = [got_c, hop(got_q, PERM_C), hop(got_p, PERM_C), hop(got_r, PERM_C)]
            return [v, got_q, got_p, got_r] + cross

        def origins(first, second):
            steps = [0, first, second, first + second]
            return jnp.stack([me ^ n for n in steps] + [me ^ (n + 1) for n in steps]).astype(jnp.int32)

        same = lambda d: d
        blocks = spread_list(down1, PERM_X, PERM_Y)
        g_down = place_list(None, blocks, origins(2, 4), down_shape, 1)
        g_up = place(None, spread(up1), up_shape, 1, same)
        blocks = spread_list(down0, PERM_Y, PERM_X)
        g_down = place_list(g_down, blocks, owned(origins(4, 2)), down_shape, 0)
        g_up = place(g_up, spread(up0[0]), up_shape, 0, owned)
        g_up = place(g_up, spread(up0[1]), up_shape, 0, owned, last)

        small = jnp.concatenate([dot_tn(u0, dz0), dot_tn(o0, s0), dot_tn(u1, dz1), dot_tn(o1, s1)], axis=1)
        small = lax.optimization_barrier(small)
        acc = small.reshape(2, 2, 2, dim // shards, 4 * emb)

        def fold(v, at, axis, perm):
            got = hop(cut(v, 1 - at, 1, axis).astype(BF), perm)
            return cut(v, at, 1, axis) + got.astype(F32)

        acc = fold(acc, core, 2, PERM_C)
        acc = fold(acc, x_at, 1, PERM_X)
        acc = fold(acc, y_at, 0, PERM_Y)
        full = spread(acc.reshape(dim // shards, 4 * emb).astype(BF)).reshape(dim, 4 * emb).astype(F32)
        g_gate = jnp.stack([full[:, :emb], full[:, 2 * emb : 3 * emb]])
        g_proj = jnp.stack([full[:, emb : 2 * emb].T, full[:, 3 * emb :].T])

        all_rows, all_ids = [], []
        for l, rows in ((0, rows0), (1, rows1)):
            send = jnp.zeros((shards * cap, emb), F32).at[dest_slot].set(rows)
            all_rows.append(lax.all_to_all(send, ALL, 0, 0, tiled=True))
            all_ids.append(req_recv + l * rows_dev)
        g_tab = jax.ops.segment_sum(jnp.concatenate(all_rows), jnp.concatenate(all_ids), num_segments=layers * rows_dev)
        g_tab = g_tab.reshape(layers, rows_dev, emb)

        a1 = gelu(h1).astype(BF)
        m1 = dot_nn(a1, w_down[1]).astype(BF)
        q1 = keep(dot_nn(s1, w_proj[1]).astype(BF))
        x_out = (x1w + m1.astype(F32) + q1.astype(F32)).astype(BF)
        return x_out, g_tab, g_up, g_down, g_gate, g_proj

    grid = jax.sharding.Mesh(mesh.devices.reshape(2, 2, 2), ALL)
    return jax.shard_map(
        device_step,
        mesh=grid,
        in_specs=(P(ALL), P(ALL, None), P(ALL, None), P(None, ALL, None), P(), P(), P(), P()),
        out_specs=(P(ALL, None), P(None, ALL, None), P(), P(), P(), P()),
        check_vma=False,
    )
```
